256 devices in a mesh: rows: 64 (over z, y, core), cols: 4 (over x).
Axes of the slice: x: 4, y: 4, z: 8, core: 2. Of those that a mesh axis runs over, the one named last changes fastest.
Arguments:
- gradients: float32 [256, 128, 4096], P(None, 'rows', 'cols'), may hold values from -6 to 6
- momentum: float32 [256, 128, 4096], P(None, 'rows', 'cols'), may hold values from -6 to 6
- weights: float32 [256, 128, 4096], P(None, 'rows', 'cols'), may hold values from -0.1875 to 0.1875
Outputs:
- new_weights: float32 [256, 128, 4096], P(None, 'rows', 'cols')
- new_momentum: float32 [256, 128, 4096], P(None, 'rows', 'cols')
The draws below stay inside these ranges and needn't reach their ends.
All inputs are finite; a program needn't handle non-finite values.
Results may differ from the reference program's by a relative error of at most 0.0003.
Values sent between devices are 32-bit elements.
A program may use at most 64 MiB of HBM per device.

```python
import jax
import jax.numpy as jnp
from jax import lax

SIDE = 128
WIDE = 4096
MATS = 256
ITERS = 4


def level_of(stream_key, dims, pieces, least, largest):
    def one(dim, blocks):
        steps = jax.random.uniform(jax.random.fold_in(jax.random.fold_in(stream_key, 6), dim), (blocks,), jnp.float32, least / len(pieces), largest / len(pieces))
        return jnp.repeat(jnp.exp(steps), dims[dim] // blocks).reshape((-1,) + (1,) * (len(dims) - dim - 1))

    gain = one(*pieces[0])
    for cut in pieces[1:]:
        gain = gain * one(*cut)
    return gain


def noise(stream_key, extent, scale, limit, cuts=(), kind=jnp.bfloat16):
    result = scale * jax.random.normal(stream_key, extent, jnp.float32)
    if cuts:
        result = result * level_of(stream_key, extent, cuts, -0.22, 0.18)
    return jnp.clip(result, -limit, limit).astype(kind)


def setup_inputs(seed: int = 0) -> dict:
    streams_of = jax.random.split(jax.random.key(seed), 4)
    return {
        "gradients": noise(streams_of[0], (MATS, SIDE, WIDE), 1.0, 6.0, ((1, 64), (2, 4)), jnp.float32),
        "momentum": noise(streams_of[1], (MATS, SIDE, WIDE), 1.0, 6.0, ((1, 64), (2, 4)), jnp.float32),
        "weights": noise(streams_of[2], (MATS, SIDE, WIDE), 0.03, 0.1875, ((1, 64), (2, 4)), jnp.float32),
    }


hold_rate = 0.8
learn_rate = 0.8
decay_rate = 0.1

def reference(gradients, momentum, weights):
    new_momentum = hold_rate * momentum + gradients

    def orthogonal_one(stack):
        iterate = stack[None]
        iterate = iterate * lax.rsqrt(lax.optimization_barrier(jnp.sum(iterate * iterate, axis=(1, 2), keepdims=True)) + 1e-06)
        for step in range(ITERS):
            gram = jnp.einsum('mik,mjk->mij', iterate, iterate, precision=lax.Precision.HIGHEST)
            mixed = -4.775 * gram + 2.0315 * jnp.einsum('mij,mjk->mik', gram, gram, precision=lax.Precision.HIGHEST)
            iterate = 3.4445 * iterate + jnp.einsum('mij,mjk->mik', mixed, iterate, precision=lax.Precision.HIGHEST)
        return iterate[0]
    iterate = lax.map(orthogonal_one, new_momentum)
    new_weights = (1.0 - learn_rate * decay_rate) * weights - learn_rate * iterate
    return (new_weights, new_momentum)
```

```python
import functools

import jax
import jax.numpy as jnp
from jax import lax
from jax.experimental import pallas as pl
from jax.experimental.pallas import tpu as pltpu
from jax.sharding import PartitionSpec as P

ITERS = 4
hold_rate = 0.8
learn_rate = 0.8
decay_rate = 0.1

MESH = pl.DeviceIdType.MESH
HIGHEST = lax.Precision.HIGHEST

ROWS = 64
COLS = 4
SIDE = 128
LANES = 128
TILES = 8
PIECE = 2 * TILES
HELD = 4
STAGES = 2
PER = HELD // STAGES
BLOCK = PER * PIECE
FLAT = ROWS * HELD * PIECE
STEPS = (27, 43)


def dot(a, b, dims=(((1,), (0,)), ((), ()))):
    return lax.dot_general(a, b, dims, precision=HIGHEST, preferred_element_type=jnp.float32)


def mixing(gram):
    row = lax.broadcasted_iota(jnp.int32, (SIDE, SIDE), 0)
    col = lax.broadcasted_iota(jnp.int32, (SIDE, SIDE), 1)
    eye = row == col
    total = jnp.sum(jnp.sum(jnp.where(eye, gram, 0.0), axis=1, keepdims=True), axis=0, keepdims=True)
    scale = lax.rsqrt(total + 1e-06)
    a = gram * scale * scale
    q = None
    for step in range(ITERS):
        b = -4.775 * a + 2.0315 * dot(a, a)
        if q is None:
            q = (jnp.where(eye, 3.4445, 0.0) + b) * scale
        else:
            q = 3.4445 * q + dot(b, q)
        if step < ITERS - 1:
            half = 3.4445 * a + dot(a, b)
            a = 3.4445 * half + dot(b, half)
    return q


def kernel(
    g_hbm, m_hbm, w_hbm, nw_ref, nm_ref,
    g_buf, m_buf, w_buf, taken, spread, back, whole, part, parts, mixer,
    load_sem, in_send, in_recv, out_send, out_recv, part_send, part_recv, mix_send, mix_recv,
):
    me = lax.axis_index("rows")
    col = lax.axis_index("cols")
    z, y, core = me // 8, (me // 2) % 4, me % 2

    def peer(j, step):
        off = (j * step) % ROWS
        dz, dy, dc = off // 8, (off // 2) % 4, off % 2
        return ((z + dz) % 8) * 8 + ((y + dy) % 4) * 2 + (core + dc) % 2

    half = FLAT // 2
    loads = []
    for i, (src, dst) in enumerate(((g_hbm, g_buf), (m_hbm, m_buf), (w_hbm, w_buf))):
        load = pltpu.make_async_copy(src, dst, load_sem.at[i])
        load.start()
        loads.append(load)

    barrier = pltpu.get_barrier_semaphore()

    def greet(j, carry):
        pl.semaphore_signal(barrier, inc=1, device_id={"rows": peer(j, STEPS[0])}, device_id_type=MESH)
        return carry

    lax.fori_loop(1, ROWS, greet, 0)
    for d in range(1, COLS):
        pl.semaphore_signal(barrier, inc=1, device_id={"cols": (col + d) % COLS}, device_id_type=MESH)

    loads[0].wait()
    loads[1].wait()

    def hold(i, carry):
        at = pl.ds(pl.multiple_of(i * 64, 64), 64)
        nm_ref[at, :] = hold_rate * m_buf[at, :] + g_buf[at, :]
        return carry

    lax.fori_loop(0, FLAT // 64, hold, 0, unroll=4)

    pl.semaphore_wait(barrier, ROWS - 1 + COLS - 1)

    def block(owner, s):
        return pl.ds(pl.multiple_of(owner * (HELD * PIECE) + s * BLOCK, BLOCK), BLOCK)

    def slot(owner):
        return pl.ds(pl.multiple_of(owner * BLOCK, BLOCK), BLOCK)

    for s in range(STAGES):

        def send_in(j, carry, s=s):
            to = peer(j, STEPS[s % 2])
            pltpu.make_async_remote_copy(
                src_ref=nm_ref.at[block(to, s)],
                dst_ref=taken.at[s, slot(me)],
                send_sem=in_send.at[s],
                recv_sem=in_recv.at[s],
                device_id={"rows": to},
                device_id_type=MESH,
            ).start()
            return carry

        lax.fori_loop(1, ROWS, send_in, 0)
    for s in range(STAGES):
        taken[s, slot(me), :] = nm_ref[block(me, s), :]

    def wait_all(ref, rows, sem):
        at = ref.at[pl.ds(0, rows)]
        pltpu.make_async_copy(at, at, sem).wait()

    def grams(s):
        wait_all(taken.at[s], (ROWS - 1) * BLOCK, in_recv.at[s])
        for i in range(PER):
            k = s * PER + i
            for t in range(TILES):
                for r in range(2):
                    whole[k, pl.ds(r * ROWS, ROWS), pl.ds(t * LANES, LANES)] = taken[
                        s, pl.ds(i * PIECE + 2 * t + r, ROWS, stride=BLOCK), :
                    ]
            x = whole[k]
            gram = dot(x, x, (((1,), (1,)), ((), ())))

            @pl.when(col == k)
            def _():
                parts[k] = gram

            @pl.when(col != k)
            def _():
                part[k] = gram
                pltpu.make_async_remote_copy(
                    src_ref=part.at[k],
                    dst_ref=parts.at[col],
                    send_sem=part_send,
                    recv_sem=part_recv,
                    device_id={"cols": k},
                    device_id_type=MESH,
                ).start()

    def mix(s):
        @pl.when(col // PER == s)
        def _():
            wait_all(part, COLS - 1, part_recv)
            mixer[col] = mixing((parts[0] + parts[1]) + (parts[2] + parts[3]))
            for d in range(1, COLS):
                pltpu.make_async_remote_copy(
                    src_ref=mixer.at[col],
                    dst_ref=mixer.at[col],
                    send_sem=mix_send,
                    recv_sem=mix_recv.at[col],
                    device_id={"cols": (col + d) % COLS},
                    device_id_type=MESH,
                ).start()

    def give(s):
        for i in range(PER):
            k = s * PER + i

            @pl.when(col != k)
            def _():
                pltpu.make_async_copy(mixer.at[k], mixer.at[k], mix_recv.at[k]).wait()

            out = dot(mixer[k], whole[k])
            for t in range(TILES):
                for r in range(2):
                    spread[s, pl.ds(i * PIECE + 2 * t + r, ROWS, stride=BLOCK), :] = out[
                        r * ROWS : (r + 1) * ROWS, t * LANES : (t + 1) * LANES
                    ]

        def send_out(j, carry):
            to = peer(j, STEPS[s % 2])
            pltpu.make_async_remote_copy(
                src_ref=spread.at[s, slot(to)],
                dst_ref=back.at[block(me, s)],
                send_sem=out_send.at[s],
                recv_sem=out_recv.at[s],
                device_id={"rows": to},
                device_id_type=MESH,
            ).start()
            return carry

        lax.fori_loop(1, ROWS, send_out, 0)
        back[block(me, s), :] = spread[s, slot(me), :]

    for s in range(STAGES):
        grams(s)
        mix(s)
        if s:
            give(s - 1)
    give(STAGES - 1)

    loads[2].wait()
    for s in range(STAGES):
        wait_all(back, (ROWS - 1) * BLOCK, out_recv.at[s])

        def decay(r, carry, s=s):
            at = block(r, s)
            nw_ref[at, :] = (1.0 - learn_rate * decay_rate) * w_buf[at, :] - learn_rate * back[at, :]
            return carry

        lax.fori_loop(0, ROWS, decay, 0, unroll=4)

    for s in range(STAGES):
        wait_all(back, (ROWS - 1) * BLOCK, in_send.at[s])
        wait_all(back, (ROWS - 1) * BLOCK, out_send.at[s])
    wait_all(part, COLS - 1, part_send)
    wait_all(part, COLS - 1, mix_send)


def flat(a):
    return a.reshape(ROWS * HELD, 2, TILES, LANES).transpose(0, 2, 1, 3).reshape(FLAT, LANES)


def square(a):
    return a.reshape(ROWS * HELD, TILES, 2, LANES).transpose(0, 2, 1, 3).reshape(ROWS * HELD, 2, TILES * LANES)


def local(gradients, momentum, weights):
    f32 = jnp.float32
    in_hbm = [pltpu.with_memory_space_constraint(flat(a), pltpu.HBM) for a in (gradients, momentum, weights)]
    vmem = pltpu.VMEM
    dma = pltpu.SemaphoreType.DMA
    new_weights, new_momentum = pl.pallas_call(
        kernel,
        out_shape=[pltpu.VMEM((FLAT, LANES), f32)] * 2,
        in_specs=[pl.BlockSpec(memory_space=pltpu.HBM)] * 3,
        scratch_shapes=[
            vmem((FLAT, LANES), f32),
            vmem((FLAT, LANES), f32),
            vmem((FLAT, LANES), f32),
            vmem((STAGES, ROWS * BLOCK, LANES), f32),
            vmem((STAGES, ROWS * BLOCK, LANES), f32),
            vmem((FLAT, LANES), f32),
            vmem((HELD, SIDE, TILES * LANES), f32),
            vmem((HELD, SIDE, SIDE), f32),
            vmem((COLS, SIDE, SIDE), f32),
            vmem((HELD, SIDE, SIDE), f32),
            dma((3,)),
            dma((STAGES,)),
            dma((STAGES,)),
            dma((STAGES,)),
            dma((STAGES,)),
            dma(()),
            dma(()),
            dma(()),
            dma((HELD,)),
        ],
        compiler_params=pltpu.CompilerParams(
            collective_id=0, has_side_effects=True, vmem_limit_bytes=40 * 2**20
        ),
        name="step",
    )(*in_hbm)
    return square(new_weights), square(new_momentum)


def solution(mesh):
    placed = P(None, "rows", "cols")
    return jax.shard_map(
        local, mesh=mesh, in_specs=(placed, placed, placed), out_specs=(placed, placed), check_vma=False
    )
```

```python
import functools

import jax
import jax.numpy as jnp
from jax import lax
from jax.experimental import pallas as pl
from jax.experimental.pallas import tpu as pltpu
from jax.sharding import PartitionSpec as P

ITERS = 4
hold_rate = 0.8
learn_rate = 0.8
decay_rate = 0.1

MESH = pl.DeviceIdType.MESH
HIGHEST = lax.Precision.HIGHEST

ROWS = 64
COLS = 4
SIDE = 128
LANES = 128
TILES = 8
PIECE = 2 * TILES
HELD = 4
STAGES = 4
PER = HELD // STAGES
BLOCK = PER * PIECE
FLAT = ROWS * HELD * PIECE
STEPS = (27, 43)


def dot(a, b, dims=(((1,), (0,)), ((), ()))):
    return lax.dot_general(a, b, dims, precision=HIGHEST, preferred_element_type=jnp.float32)


def mixing(gram):
    row = lax.broadcasted_iota(jnp.int32, (SIDE, SIDE), 0)
    col = lax.broadcasted_iota(jnp.int32, (SIDE, SIDE), 1)
    eye = row == col
    total = jnp.sum(jnp.sum(jnp.where(eye, gram, 0.0), axis=1, keepdims=True), axis=0, keepdims=True)
    scale = lax.rsqrt(total + 1e-06)
    a = gram * scale * scale
    q = None
    for step in range(ITERS):
        b = -4.775 * a + 2.0315 * dot(a, a)
        if q is None:
            q = (jnp.where(eye, 3.4445, 0.0) + b) * scale
        else:
            q = 3.4445 * q + dot(b, q)
        if step < ITERS - 1:
            half = 3.4445 * a + dot(a, b)
            a = 3.4445 * half + dot(b, half)
    return q


def kernel(
    g_hbm, m_hbm, w_hbm, nw_ref, nm_ref,
    g_buf, m_buf, w_buf, taken, spread, back, whole, part, parts, mixer,
    load_sem, in_send, in_recv, out_send, out_recv, part_send, part_recv, mix_send, mix_recv,
):
    me = lax.axis_index("rows")
    col = lax.axis_index("cols")
    z, y, core = me // 8, (me // 2) % 4, me % 2

    def peer(j, step):
        off = (j * step) % ROWS
        dz, dy, dc = off // 8, (off // 2) % 4, off % 2
        return ((z + dz) % 8) * 8 + ((y + dy) % 4) * 2 + (core + dc) % 2

    half = FLAT // 2
    loads = []
    for i, (src, dst) in enumerate(((g_hbm, g_buf), (m_hbm, m_buf), (w_hbm, w_buf))):
        load = pltpu.make_async_copy(src, dst, load_sem.at[i])
        load.start()
        loads.append(load)

    barrier = pltpu.get_barrier_semaphore()

    def greet(j, carry):
        pl.semaphore_signal(barrier, inc=1, device_id={"rows": peer(j, STEPS[0])}, device_id_type=MESH)
        return carry

    lax.fori_loop(1, ROWS, greet, 0)
    for d in range(1, COLS):
        pl.semaphore_signal(barrier, inc=1, device_id={"cols": (col + d) % COLS}, device_id_type=MESH)

    loads[0].wait()
    loads[1].wait()

    def hold(i, carry):
        at = pl.ds(pl.multiple_of(i * 64, 64), 64)
        nm_ref[at, :] = hold_rate * m_buf[at, :] + g_buf[at, :]
        return carry

    lax.fori_loop(0, FLAT // 64, hold, 0, unroll=4)

    pl.semaphore_wait(barrier, ROWS - 1 + COLS - 1)

    def block(owner, s):
        return pl.ds(pl.multiple_of(owner * (HELD * PIECE) + s * BLOCK, BLOCK), BLOCK)

    def slot(owner):
        return pl.ds(pl.multiple_of(owner * BLOCK, BLOCK), BLOCK)

    for s in range(STAGES):

        def send_in(j, carry, s=s):
            to = peer(j, STEPS[s % 2])
            pltpu.make_async_remote_copy(
                src_ref=nm_ref.at[block(to, s)],
                dst_ref=taken.at[s, slot(me)],
                send_sem=in_send.at[s],
                recv_sem=in_recv.at[s],
                device_id={"rows": to},
                device_id_type=MESH,
            ).start()
            return carry

        lax.fori_loop(1, ROWS, send_in, 0)
    for s in range(STAGES):
        taken[s, slot(me), :] = nm_ref[block(me, s), :]

    def wait_all(ref, rows, sem):
        at = ref.at[pl.ds(0, rows)]
        pltpu.make_async_copy(at, at, sem).wait()

    def grams(s):
        wait_all(taken.at[s], (ROWS - 1) * BLOCK, in_recv.at[s])
        for i in range(PER):
            k = s * PER + i
            for t in range(TILES):
                for r in range(2):
                    whole[k, pl.ds(r * ROWS, ROWS), pl.ds(t * LANES, LANES)] = taken[
                        s, pl.ds(i * PIECE + 2 * t + r, ROWS, stride=BLOCK), :
                    ]
            x = whole[k]
            gram = dot(x, x, (((1,), (1,)), ((), ())))

            @pl.when(col == k)
            def _():
                parts[k] = gram

            @pl.when(col != k)
            def _():
                part[k] = gram
                pltpu.make_async_remote_copy(
                    src_ref=part.at[k],
                    dst_ref=parts.at[col],
                    send_sem=part_send,
                    recv_sem=part_recv,
                    device_id={"cols": k},
                    device_id_type=MESH,
                ).start()

    def mix(s):
        @pl.when(col // PER == s)
        def _():
            wait_all(part, COLS - 1, part_recv)
            mixer[col] = mixing((parts[0] + parts[1]) + (parts[2] + parts[3]))
            for d in range(1, COLS):
                pltpu.make_async_remote_copy(
                    src_ref=mixer.at[col],
                    dst_ref=mixer.at[col],
                    send_sem=mix_send,
                    recv_sem=mix_recv.at[col],
                    device_id={"cols": (col + d) % COLS},
                    device_id_type=MESH,
                ).start()

    def give(s):
        for i in range(PER):
            k = s * PER + i

            @pl.when(col != k)
            def _():
                pltpu.make_async_copy(mixer.at[k], mixer.at[k], mix_recv.at[k]).wait()

            out = dot(mixer[k], whole[k])
            for t in range(TILES):
                for r in range(2):
                    spread[s, pl.ds(i * PIECE + 2 * t + r, ROWS, stride=BLOCK), :] = out[
                        r * ROWS : (r + 1) * ROWS, t * LANES : (t + 1) * LANES
                    ]

        def send_out(j, carry):
            to = peer(j, STEPS[s % 2])
            pltpu.make_async_remote_copy(
                src_ref=spread.at[s, slot(to)],
                dst_ref=back.at[block(me, s)],
                send_sem=out_send.at[s],
                recv_sem=out_recv.at[s],
                device_id={"rows": to},
                device_id_type=MESH,
            ).start()
            return carry

        lax.fori_loop(1, ROWS, send_out, 0)
        back[block(me, s), :] = spread[s, slot(me), :]

    for s in range(STAGES):
        grams(s)
        mix(s)
        give(s)

    loads[2].wait()
    for s in range(STAGES):
        wait_all(back, (ROWS - 1) * BLOCK, out_recv.at[s])

        def decay(r, carry, s=s):
            at = block(r, s)
            nw_ref[at, :] = (1.0 - learn_rate * decay_rate) * w_buf[at, :] - learn_rate * back[at, :]
            return carry

        lax.fori_loop(0, ROWS, decay, 0, unroll=4)

    for s in range(STAGES):
        wait_all(back, (ROWS - 1) * BLOCK, in_send.at[s])
        wait_all(back, (ROWS - 1) * BLOCK, out_send.at[s])
    wait_all(part, COLS - 1, part_send)
    wait_all(part, COLS - 1, mix_send)


def flat(a):
    return a.reshape(ROWS * HELD, 2, TILES, LANES).transpose(0, 2, 1, 3).reshape(FLAT, LANES)


def square(a):
    return a.reshape(ROWS * HELD, TILES, 2, LANES).transpose(0, 2, 1, 3).reshape(ROWS * HELD, 2, TILES * LANES)


def local(gradients, momentum, weights):
    f32 = jnp.float32
    in_hbm = [pltpu.with_memory_space_constraint(flat(a), pltpu.HBM) for a in (gradients, momentum, weights)]
    vmem = pltpu.VMEM
    dma = pltpu.SemaphoreType.DMA
    new_weights, new_momentum = pl.pallas_call(
        kernel,
        out_shape=[pltpu.VMEM((FLAT, LANES), f32)] * 2,
        in_specs=[pl.BlockSpec(memory_space=pltpu.HBM)] * 3,
        scratch_shapes=[
            vmem((FLAT, LANES), f32),
            vmem((FLAT, LANES), f32),
            vmem((FLAT, LANES), f32),
            vmem((STAGES, ROWS * BLOCK, LANES), f32),
            vmem((STAGES, ROWS * BLOCK, LANES), f32),
            vmem((FLAT, LANES), f32),
            vmem((HELD, SIDE, TILES * LANES), f32),
            vmem((HELD, SIDE, SIDE), f32),
            vmem((COLS, SIDE, SIDE), f32),
            vmem((HELD, SIDE, SIDE), f32),
            dma((3,)),
            dma((STAGES,)),
            dma((STAGES,)),
            dma((STAGES,)),
            dma((STAGES,)),
            dma(()),
            dma(()),
            dma(()),
            dma((HELD,)),
        ],
        compiler_params=pltpu.CompilerParams(
            collective_id=0, has_side_effects=True, vmem_limit_bytes=40 * 2**20
        ),
        name="step",
    )(*in_hbm)
    return square(new_weights), square(new_momentum)


def solution(mesh):
    placed = P(None, "rows", "cols")
    return jax.shard_map(
        local, mesh=mesh, in_specs=(placed, placed, placed), out_specs=(placed, placed), check_vma=False
    )
```

```python
import functools

import jax
import jax.numpy as jnp
from jax import lax
from jax.experimental import pallas as pl
from jax.experimental.pallas import tpu as pltpu
from jax.sharding import PartitionSpec as P

ITERS = 4
hold_rate = 0.8
learn_rate = 0.8
decay_rate = 0.1

MESH = pl.DeviceIdType.MESH
HIGHEST = lax.Precision.HIGHEST

DEPTH = 8
PLANE = 8
ROWS = DEPTH * PLANE
COLS = 4
SIDE = 128
LANES = 128
TILES = 8
PIECE = 2 * TILES
HELD = 4
STAGES = 4
PER = HELD // STAGES
BLOCK = PER * PIECE
FLAT = ROWS * HELD * PIECE
STEPS = (27, 43)


def dot(a, b, dims=(((1,), (0,)), ((), ()))):
    return lax.dot_general(a, b, dims, precision=HIGHEST, preferred_element_type=jnp.float32)


def mixing(gram):
    row = lax.broadcasted_iota(jnp.int32, (SIDE, SIDE), 0)
    col = lax.broadcasted_iota(jnp.int32, (SIDE, SIDE), 1)
    eye = row == col
    total = jnp.sum(jnp.sum(jnp.where(eye, gram, 0.0), axis=1, keepdims=True), axis=0, keepdims=True)
    scale = lax.rsqrt(total + 1e-06)
    a = gram * scale * scale
    q = None
    for step in range(ITERS):
        b = -4.775 * a + 2.0315 * dot(a, a)
        if q is None:
            q = (jnp.where(eye, 3.4445, 0.0) + b) * scale
        else:
            q = 3.4445 * q + dot(b, q)
        if step < ITERS - 1:
            half = 3.4445 * a + dot(a, b)
            a = 3.4445 * half + dot(b, half)
    return q


def kernel(
    g_hbm, m_hbm, w_hbm, nw_ref, nm_ref,
    g_buf, m_buf, w_buf, taken, spread, back, whole, part, parts, mixer,
    load_sem, in_send, in_recv, out_send, out_recv, part_send, part_recv, mix_send, mix_recv, below, above,
):
    me = lax.axis_index("rows")
    col = lax.axis_index("cols")
    z, y, core = me // 8, (me // 2) % 4, me % 2

    def peer(j, step):
        off = (j * step) % ROWS
        dz, dy, dc = off // 8, (off // 2) % 4, off % 2
        return ((z + dz) % 8) * 8 + ((y + dy) % 4) * 2 + (core + dc) % 2

    half = FLAT // 2
    loads = []
    for i, (src, dst) in enumerate(((g_hbm, g_buf), (m_hbm, m_buf), (w_hbm, w_buf))):
        load = pltpu.make_async_copy(src, dst, load_sem.at[i])
        load.start()
        loads.append(load)

    barrier = pltpu.get_barrier_semaphore()

    def away(dz, j):
        return ((z + dz) % DEPTH) * PLANE + (me + j) % PLANE

    def greet(dz, j):
        pl.semaphore_signal(barrier, inc=1, device_id={"rows": away(dz, j)}, device_id_type=MESH)

    @pl.loop(0, PLANE)
    def _(j):
        greet(DEPTH - 1, j)
        greet(1, j)

    @pl.loop(1, PLANE)
    def _(j):
        greet(0, j)

    for d in range(1, COLS):
        pl.semaphore_signal(barrier, inc=1, device_id={"cols": (col + d) % COLS}, device_id_type=MESH)

    loads[0].wait()
    loads[1].wait()

    def hold(i, carry):
        at = pl.ds(pl.multiple_of(i * 64, 64), 64)
        nm_ref[at, :] = hold_rate * m_buf[at, :] + g_buf[at, :]
        return carry

    lax.fori_loop(0, FLAT // 64, hold, 0, unroll=4)

    pl.semaphore_wait(barrier, 3 * PLANE - 1 + COLS - 1)

    def tell():
        pl.semaphore_signal(below, inc=1, device_id={"rows": away(1, 0)}, device_id_type=MESH)
        pl.semaphore_signal(above, inc=1, device_id={"rows": away(DEPTH - 1, 0)}, device_id_type=MESH)

    def hear():
        pl.semaphore_wait(below, 1)
        pl.semaphore_wait(above, 1)

    tell()

    def block(owner, s):
        return pl.ds(pl.multiple_of(owner * (HELD * PIECE) + s * BLOCK, BLOCK), BLOCK)

    def slot(owner):
        return pl.ds(pl.multiple_of(owner * BLOCK, BLOCK), BLOCK)

    def send_in(to, s):
        pltpu.make_async_remote_copy(
            src_ref=nm_ref.at[block(to, s)],
            dst_ref=taken.at[s, slot(me)],
            send_sem=in_send.at[s],
            recv_sem=in_recv.at[s],
            device_id={"rows": to},
            device_id_type=MESH,
        ).start()

    for dz in range(1, DEPTH // 2 + 1):
        if dz > 1:
            hear()
            if dz < DEPTH // 2:
                tell()

        @pl.loop(0, PLANE)
        def _(j, dz=dz):
            send_in(away(dz, j), 0)
            if dz < DEPTH // 2:
                send_in(away(DEPTH - dz, j), 0)

        if dz == 1:

            @pl.loop(1, PLANE)
            def _(j):
                send_in(away(0, j), 0)

    for s in range(1, STAGES):

        @pl.loop(1, ROWS)
        def _(j, s=s):
            send_in(peer(j, STEPS[s % 2]), s)

    for s in range(STAGES):
        taken[s, slot(me), :] = nm_ref[block(me, s), :]

    def wait_all(ref, rows, sem):
        at = ref.at[pl.ds(0, rows)]
        pltpu.make_async_copy(at, at, sem).wait()

    def grams(s):
        wait_all(taken.at[s], (ROWS - 1) * BLOCK, in_recv.at[s])
        for i in range(PER):
            k = s * PER + i
            for t in range(TILES):
                for r in range(2):
                    whole[k, pl.ds(r * ROWS, ROWS), pl.ds(t * LANES, LANES)] = taken[
                        s, pl.ds(i * PIECE + 2 * t + r, ROWS, stride=BLOCK), :
                    ]
            x = whole[k]
            gram = dot(x, x, (((1,), (1,)), ((), ())))

            @pl.when(col == k)
            def _():
                parts[k] = gram

            @pl.when(col != k)
            def _():
                part[k] = gram
                pltpu.make_async_remote_copy(
                    src_ref=part.at[k],
                    dst_ref=parts.at[col],
                    send_sem=part_send,
                    recv_sem=part_recv,
                    device_id={"cols": k},
                    device_id_type=MESH,
                ).start()

    def mix(s):
        @pl.when(col // PER == s)
        def _():
            wait_all(part, COLS - 1, part_recv)
            mixer[col] = mixing((parts[0] + parts[1]) + (parts[2] + parts[3]))
            for d in range(1, COLS):
                pltpu.make_async_remote_copy(
                    src_ref=mixer.at[col],
                    dst_ref=mixer.at[col],
                    send_sem=mix_send,
                    recv_sem=mix_recv.at[col],
                    device_id={"cols": (col + d) % COLS},
                    device_id_type=MESH,
                ).start()

    def give(s):
        for i in range(PER):
            k = s * PER + i

            @pl.when(col != k)
            def _():
                pltpu.make_async_copy(mixer.at[k], mixer.at[k], mix_recv.at[k]).wait()

            out = dot(mixer[k], whole[k])
            for t in range(TILES):
                for r in range(2):
                    spread[s, pl.ds(i * PIECE + 2 * t + r, ROWS, stride=BLOCK), :] = out[
                        r * ROWS : (r + 1) * ROWS, t * LANES : (t + 1) * LANES
                    ]

        def send_out(j, carry):
            to = peer(j, STEPS[s % 2])
            pltpu.make_async_remote_copy(
                src_ref=spread.at[s, slot(to)],
                dst_ref=back.at[block(me, s)],
                send_sem=out_send.at[s],
                recv_sem=out_recv.at[s],
                device_id={"rows": to},
                device_id_type=MESH,
            ).start()
            return carry

        lax.fori_loop(1, ROWS, send_out, 0)
        back[block(me, s), :] = spread[s, slot(me), :]

    for s in range(STAGES):
        grams(s)
        mix(s)
        give(s)

    loads[2].wait()
    for s in range(STAGES):
        wait_all(back, (ROWS - 1) * BLOCK, out_recv.at[s])

        def decay(r, carry, s=s):
            at = block(r, s)
            nw_ref[at, :] = (1.0 - learn_rate * decay_rate) * w_buf[at, :] - learn_rate * back[at, :]
            return carry

        lax.fori_loop(0, ROWS, decay, 0, unroll=4)

    for s in range(STAGES):
        wait_all(back, (ROWS - 1) * BLOCK, in_send.at[s])
        wait_all(back, (ROWS - 1) * BLOCK, out_send.at[s])
    wait_all(part, COLS - 1, part_send)
    wait_all(part, COLS - 1, mix_send)


def store(nw_ref, nm_ref, nw_hbm, nm_hbm, sem):
    copies = [
        pltpu.make_async_copy(nw_ref, nw_hbm, sem.at[0]),
        pltpu.make_async_copy(nm_ref, nm_hbm, sem.at[1]),
    ]
    for copy in copies:
        copy.start()
    for copy in copies:
        copy.wait()


def flat(a):
    return a.reshape(ROWS * HELD, 2, TILES, LANES).transpose(0, 2, 1, 3).reshape(FLAT, LANES)


def square(a):
    return a.reshape(ROWS * HELD, TILES, 2, LANES).transpose(0, 2, 1, 3).reshape(ROWS * HELD, 2, TILES * LANES)


def local(gradients, momentum, weights):
    f32 = jnp.float32
    in_hbm = [pltpu.with_memory_space_constraint(flat(a), pltpu.HBM) for a in (gradients, momentum, weights)]
    vmem = pltpu.VMEM
    dma = pltpu.SemaphoreType.DMA
    new_weights, new_momentum = pl.pallas_call(
        kernel,
        out_shape=[pltpu.VMEM((FLAT, LANES), f32)] * 2,
        in_specs=[pl.BlockSpec(memory_space=pltpu.HBM)] * 3,
        scratch_shapes=[
            vmem((FLAT, LANES), f32),
            vmem((FLAT, LANES), f32),
            vmem((FLAT, LANES), f32),
            vmem((STAGES, ROWS * BLOCK, LANES), f32),
            vmem((STAGES, ROWS * BLOCK, LANES), f32),
            vmem((FLAT, LANES), f32),
            vmem((HELD, SIDE, TILES * LANES), f32),
            vmem((HELD, SIDE, SIDE), f32),
            vmem((COLS, SIDE, SIDE), f32),
            vmem((HELD, SIDE, SIDE), f32),
            dma((3,)),
            dma((STAGES,)),
            dma((STAGES,)),
            dma((STAGES,)),
            dma((STAGES,)),
            dma(()),
            dma(()),
            dma(()),
            dma((HELD,)),
            pltpu.SemaphoreType.REGULAR,
            pltpu.SemaphoreType.REGULAR,
        ],
        compiler_params=pltpu.CompilerParams(
            collective_id=0, has_side_effects=True, vmem_limit_bytes=40 * 2**20
        ),
        name="step",
    )(*in_hbm)
    new_weights, new_momentum = pl.pallas_call(
        store,
        out_shape=[jax.ShapeDtypeStruct((FLAT, LANES), f32)] * 2,
        in_specs=[pl.BlockSpec(memory_space=pltpu.VMEM)] * 2,
        out_specs=[pl.BlockSpec(memory_space=pl.ANY)] * 2,
        scratch_shapes=[dma((2,))],
        compiler_params=pltpu.CompilerParams(vmem_limit_bytes=2**20),
        name="store",
    )(new_weights, new_momentum)
    return square(new_weights), square(new_momentum)


def solution(mesh):
    placed = P(None, "rows", "cols")
    return jax.shard_map(
        local, mesh=mesh, in_specs=(placed, placed, placed), out_specs=(placed, placed), check_vma=False
    )
```

```python
import functools

import jax
import jax.numpy as jnp
from jax import lax
from jax.experimental import pallas as pl
from jax.experimental.pallas import tpu as pltpu
from jax.sharding import PartitionSpec as P

ITERS = 4
hold_rate = 0.8
learn_rate = 0.8
decay_rate = 0.1

MESH = pl.DeviceIdType.MESH
HIGHEST = lax.Precision.HIGHEST

DEPTH = 8
PLANE = 8
ROWS = DEPTH * PLANE
COLS = 4
SIDE = 128
LANES = 128
TILES = 8
PIECE = 2 * TILES
HELD = 4
STAGES = 4
PER = HELD // STAGES
BLOCK = PER * PIECE
FLAT = ROWS * HELD * PIECE
STEPS = (13, 37)


def dot(a, b, dims=(((1,), (0,)), ((), ()))):
    return lax.dot_general(a, b, dims, precision=HIGHEST, preferred_element_type=jnp.float32)


def mixing(gram):
    row = lax.broadcasted_iota(jnp.int32, (SIDE, SIDE), 0)
    col = lax.broadcasted_iota(jnp.int32, (SIDE, SIDE), 1)
    eye = row == col
    total = jnp.sum(jnp.sum(jnp.where(eye, gram, 0.0), axis=1, keepdims=True), axis=0, keepdims=True)
    scale = lax.rsqrt(total + 1e-06)
    a = gram * scale * scale
    q = None
    for step in range(ITERS):
        b = -4.775 * a + 2.0315 * dot(a, a)
        if q is None:
            q = (jnp.where(eye, 3.4445, 0.0) + b) * scale
        else:
            q = 3.4445 * q + dot(b, q)
        if step < ITERS - 1:
            half = 3.4445 * a + dot(a, b)
            a = 3.4445 * half + dot(b, half)
    return q


def kernel(
    g_hbm, m_hbm, w_hbm, nw_ref, nm_ref,
    g_buf, m_buf, w_buf, taken, spread, back, whole, part, parts, mixer,
    load_sem, in_send, in_recv, out_send, out_recv, part_send, part_recv, mix_send, mix_recv, below, above,
):
    me = lax.axis_index("rows")
    col = lax.axis_index("cols")
    z, y, core = me // 8, (me // 2) % 4, me % 2

    def peer(j, step):
        off = (j * step) % ROWS
        dz, dy, dc = off // 8, (off // 2) % 4, off % 2
        return ((z + dz) % 8) * 8 + ((y + dy) % 4) * 2 + (core + dc) % 2

    half = FLAT // 2
    loads = []
    for i, (src, dst) in enumerate(((g_hbm, g_buf), (m_hbm, m_buf), (w_hbm, w_buf))):
        load = pltpu.make_async_copy(src, dst, load_sem.at[i])
        load.start()
        loads.append(load)

    barrier = pltpu.get_barrier_semaphore()

    def away(dz, j):
        return ((z + dz) % DEPTH) * PLANE + (me + j) % PLANE

    def far_first(send):
        for dz in range(DEPTH // 2, 0, -1):

            @pl.loop(0, PLANE)
            def _(j, dz=dz):
                send(away(dz, j))
                if dz < DEPTH // 2:
                    send(away(DEPTH - dz, j))

        @pl.loop(1, PLANE)
        def _(j):
            send(away(0, j))

    def greet(dz, j):
        pl.semaphore_signal(barrier, inc=1, device_id={"rows": away(dz, j)}, device_id_type=MESH)

    @pl.loop(0, PLANE)
    def _(j):
        greet(DEPTH - 1, j)
        greet(1, j)

    @pl.loop(1, PLANE)
    def _(j):
        greet(0, j)

    for d in range(1, COLS):
        pl.semaphore_signal(barrier, inc=1, device_id={"cols": (col + d) % COLS}, device_id_type=MESH)

    loads[0].wait()
    loads[1].wait()

    def hold(i, carry):
        at = pl.ds(pl.multiple_of(i * 64, 64), 64)
        nm_ref[at, :] = hold_rate * m_buf[at, :] + g_buf[at, :]
        return carry

    lax.fori_loop(0, FLAT // 64, hold, 0, unroll=4)

    pl.semaphore_wait(barrier, 3 * PLANE - 1 + COLS - 1)

    def tell():
        pl.semaphore_signal(below, inc=1, device_id={"rows": away(1, 0)}, device_id_type=MESH)
        pl.semaphore_signal(above, inc=1, device_id={"rows": away(DEPTH - 1, 0)}, device_id_type=MESH)

    def hear():
        pl.semaphore_wait(below, 1)
        pl.semaphore_wait(above, 1)

    tell()

    def block(owner, s):
        return pl.ds(pl.multiple_of(owner * (HELD * PIECE) + s * BLOCK, BLOCK), BLOCK)

    def slot(owner):
        return pl.ds(pl.multiple_of(owner * BLOCK, BLOCK), BLOCK)

    def send_in(to, s):
        pltpu.make_async_remote_copy(
            src_ref=nm_ref.at[block(to, s)],
            dst_ref=taken.at[s, slot(me)],
            send_sem=in_send.at[s],
            recv_sem=in_recv.at[s],
            device_id={"rows": to},
            device_id_type=MESH,
        ).start()

    for dz in range(1, DEPTH // 2 + 1):
        if dz > 1:
            hear()
            if dz < DEPTH // 2:
                tell()

        @pl.loop(0, PLANE)
        def _(j, dz=dz):
            send_in(away(dz, j), 0)
            if dz < DEPTH // 2:
                send_in(away(DEPTH - dz, j), 0)

        if dz == 1:

            @pl.loop(1, PLANE)
            def _(j):
                send_in(away(0, j), 0)

    for s in range(1, STAGES):

        @pl.loop(1, ROWS)
        def _(j, s=s):
            send_in(peer(j, STEPS[s % 2]), s)

    for s in range(STAGES):
        taken[s, slot(me), :] = nm_ref[block(me, s), :]

    def wait_all(ref, rows, sem):
        at = ref.at[pl.ds(0, rows)]
        pltpu.make_async_copy(at, at, sem).wait()

    def grams(s):
        wait_all(taken.at[s], (ROWS - 1) * BLOCK, in_recv.at[s])
        for i in range(PER):
            k = s * PER + i
            for t in range(TILES):
                for r in range(2):
                    whole[k, pl.ds(r * ROWS, ROWS), pl.ds(t * LANES, LANES)] = taken[
                        s, pl.ds(i * PIECE + 2 * t + r, ROWS, stride=BLOCK), :
                    ]
            x = whole[k]
            gram = dot(x, x, (((1,), (1,)), ((), ())))

            @pl.when(col == k)
            def _():
                parts[k] = gram

            @pl.when(col != k)
            def _():
                part[k] = gram
                pltpu.make_async_remote_copy(
                    src_ref=part.at[k],
                    dst_ref=parts.at[col],
                    send_sem=part_send,
                    recv_sem=part_recv,
                    device_id={"cols": k},
                    device_id_type=MESH,
                ).start()

    def mix(s):
        @pl.when(col // PER == s)
        def _():
            wait_all(part, COLS - 1, part_recv)
            mixer[col] = mixing((parts[0] + parts[1]) + (parts[2] + parts[3]))
            for d in range(1, COLS):
                pltpu.make_async_remote_copy(
                    src_ref=mixer.at[col],
                    dst_ref=mixer.at[col],
                    send_sem=mix_send,
                    recv_sem=mix_recv.at[col],
                    device_id={"cols": (col + d) % COLS},
                    device_id_type=MESH,
                ).start()

    def give(s):
        for i in range(PER):
            k = s * PER + i

            @pl.when(col != k)
            def _():
                pltpu.make_async_copy(mixer.at[k], mixer.at[k], mix_recv.at[k]).wait()

            out = dot(mixer[k], whole[k])
            for t in range(TILES):
                for r in range(2):
                    spread[s, pl.ds(i * PIECE + 2 * t + r, ROWS, stride=BLOCK), :] = out[
                        r * ROWS : (r + 1) * ROWS, t * LANES : (t + 1) * LANES
                    ]

        def send_out(to):
            pltpu.make_async_remote_copy(
                src_ref=spread.at[s, slot(to)],
                dst_ref=back.at[block(me, s)],
                send_sem=out_send.at[s],
                recv_sem=out_recv.at[s],
                device_id={"rows": to},
                device_id_type=MESH,
            ).start()

        if s < 3:

            @pl.loop(1, ROWS)
            def _(j):
                send_out(peer(j, STEPS[s % 2]))
        else:
            far_first(send_out)

        back[block(me, s), :] = spread[s, slot(me), :]

    for s in range(STAGES):
        grams(s)
        mix(s)
        give(s)

    loads[2].wait()
    for s in range(STAGES):
        wait_all(back, (ROWS - 1) * BLOCK, out_recv.at[s])

        def decay(r, carry, s=s):
            at = block(r, s)
            nw_ref[at, :] = (1.0 - learn_rate * decay_rate) * w_buf[at, :] - learn_rate * back[at, :]
            return carry

        lax.fori_loop(0, ROWS, decay, 0, unroll=4)

    for s in range(STAGES):
        wait_all(back, (ROWS - 1) * BLOCK, in_send.at[s])
        wait_all(back, (ROWS - 1) * BLOCK, out_send.at[s])
    wait_all(part, COLS - 1, part_send)
    wait_all(part, COLS - 1, mix_send)


def store(nw_ref, nm_ref, nw_hbm, nm_hbm, sem):
    copies = [
        pltpu.make_async_copy(nw_ref, nw_hbm, sem.at[0]),
        pltpu.make_async_copy(nm_ref, nm_hbm, sem.at[1]),
    ]
    for copy in copies:
        copy.start()
    for copy in copies:
        copy.wait()


def flat(a):
    return a.reshape(ROWS * HELD, 2, TILES, LANES).transpose(0, 2, 1, 3).reshape(FLAT, LANES)


def square(a):
    return a.reshape(ROWS * HELD, TILES, 2, LANES).transpose(0, 2, 1, 3).reshape(ROWS * HELD, 2, TILES * LANES)


def local(gradients, momentum, weights):
    f32 = jnp.float32
    in_hbm = [pltpu.with_memory_space_constraint(flat(a), pltpu.HBM) for a in (gradients, momentum, weights)]
    vmem = pltpu.VMEM
    dma = pltpu.SemaphoreType.DMA
    new_weights, new_momentum = pl.pallas_call(
        kernel,
        out_shape=[pltpu.VMEM((FLAT, LANES), f32)] * 2,
        in_specs=[pl.BlockSpec(memory_space=pltpu.HBM)] * 3,
        scratch_shapes=[
            vmem((FLAT, LANES), f32),
            vmem((FLAT, LANES), f32),
            vmem((FLAT, LANES), f32),
            vmem((STAGES, ROWS * BLOCK, LANES), f32),
            vmem((STAGES, ROWS * BLOCK, LANES), f32),
            vmem((FLAT, LANES), f32),
            vmem((HELD, SIDE, TILES * LANES), f32),
            vmem((HELD, SIDE, SIDE), f32),
            vmem((COLS, SIDE, SIDE), f32),
            vmem((HELD, SIDE, SIDE), f32),
            dma((3,)),
            dma((STAGES,)),
            dma((STAGES,)),
            dma((STAGES,)),
            dma((STAGES,)),
            dma(()),
            dma(()),
            dma(()),
            dma((HELD,)),
            pltpu.SemaphoreType.REGULAR,
            pltpu.SemaphoreType.REGULAR,
        ],
        compiler_params=pltpu.CompilerParams(
            collective_id=0, has_side_effects=True, vmem_limit_bytes=40 * 2**20
        ),
        name="step",
    )(*in_hbm)
    new_weights, new_momentum = pl.pallas_call(
        store,
        out_shape=[jax.ShapeDtypeStruct((FLAT, LANES), f32)] * 2,
        in_specs=[pl.BlockSpec(memory_space=pltpu.VMEM)] * 2,
        out_specs=[pl.BlockSpec(memory_space=pl.ANY)] * 2,
        scratch_shapes=[dma((2,))],
        compiler_params=pltpu.CompilerParams(vmem_limit_bytes=2**20),
        name="store",
    )(new_weights, new_momentum)
    return square(new_weights), square(new_momentum)


def solution(mesh):
    placed = P(None, "rows", "cols")
    return jax.shard_map(
        local, mesh=mesh, in_specs=(placed, placed, placed), out_specs=(placed, placed), check_vma=False
    )
```

```python
import functools

import jax
import jax.numpy as jnp
from jax import lax
from jax.experimental import pallas as pl
from jax.experimental.pallas import tpu as pltpu
from jax.sharding import PartitionSpec as P

ITERS = 4
hold_rate = 0.8
learn_rate = 0.8
decay_rate = 0.1

MESH = pl.DeviceIdType.MESH
HIGHEST = lax.Precision.HIGHEST

DEPTH = 8
PLANE = 8
ROWS = DEPTH * PLANE
COLS = 4
SIDE = 128
LANES = 128
TILES = 8
PIECE = 2 * TILES
HELD = 4
STAGES = 4
PER = HELD // STAGES
BLOCK = PER * PIECE
FLAT = ROWS * HELD * PIECE
STEPS = (13, 37)


def dot(a, b, dims=(((1,), (0,)), ((), ()))):
    return lax.dot_general(a, b, dims, precision=HIGHEST, preferred_element_type=jnp.float32)


def mixing(gram):
    row = lax.broadcasted_iota(jnp.int32, (SIDE, SIDE), 0)
    col = lax.broadcasted_iota(jnp.int32, (SIDE, SIDE), 1)
    eye = row == col
    total = jnp.sum(jnp.sum(jnp.where(eye, gram, 0.0), axis=1, keepdims=True), axis=0, keepdims=True)
    scale = lax.rsqrt(total + 1e-06)
    a = gram * scale * scale
    q = None
    for step in range(ITERS):
        b = -4.775 * a + 2.0315 * dot(a, a)
        if q is None:
            q = (jnp.where(eye, 3.4445, 0.0) + b) * scale
        else:
            q = 3.4445 * q + dot(b, q)
        if step < ITERS - 1:
            half = 3.4445 * a + dot(a, b)
            a = 3.4445 * half + dot(b, half)
    return q


def kernel(
    g_hbm, m_hbm, w_hbm, nw_ref, nm_ref,
    g_buf, m_buf, w_buf, taken, spread, back, whole, part, parts, mixer,
    load_sem, in_send, in_recv, out_send, out_recv, part_send, part_recv, mix_send, mix_recv, below, above,
):
    me = lax.axis_index("rows")
    col = lax.axis_index("cols")
    z, y, core = me // 8, (me // 2) % 4, me % 2

    def peer(j, step):
        off = (j * step) % ROWS
        dz, dy, dc = off // 8, (off // 2) % 4, off % 2
        return ((z + dz) % 8) * 8 + ((y + dy) % 4) * 2 + (core + dc) % 2

    half = FLAT // 2
    loads = []
    for i, (src, dst) in enumerate(((g_hbm, g_buf), (m_hbm, m_buf), (w_hbm, w_buf))):
        load = pltpu.make_async_copy(src, dst, load_sem.at[i])
        load.start()
        loads.append(load)

    barrier = pltpu.get_barrier_semaphore()

    def away(dz, j):
        return ((z + dz) % DEPTH) * PLANE + (me + j) % PLANE

    def greet(dz, j):
        pl.semaphore_signal(barrier, inc=1, device_id={"rows": away(dz, j)}, device_id_type=MESH)

    @pl.loop(0, PLANE)
    def _(j):
        greet(DEPTH - 1, j)
        greet(1, j)

    @pl.loop(1, PLANE)
    def _(j):
        greet(0, j)

    for d in range(1, COLS):
        pl.semaphore_signal(barrier, inc=1, device_id={"cols": (col + d) % COLS}, device_id_type=MESH)

    loads[0].wait()
    loads[1].wait()

    def hold(i, carry):
        at = pl.ds(pl.multiple_of(i * 64, 64), 64)
        nm_ref[at, :] = hold_rate * m_buf[at, :] + g_buf[at, :]
        return carry

    lax.fori_loop(0, FLAT // 64, hold, 0, unroll=4)

    pl.semaphore_wait(barrier, 3 * PLANE - 1 + COLS - 1)

    def tell():
        pl.semaphore_signal(below, inc=1, device_id={"rows": away(1, 0)}, device_id_type=MESH)
        pl.semaphore_signal(above, inc=1, device_id={"rows": away(DEPTH - 1, 0)}, device_id_type=MESH)

    def hear():
        pl.semaphore_wait(below, 1)
        pl.semaphore_wait(above, 1)

    tell()

    def block(owner, s):
        return pl.ds(pl.multiple_of(owner * (HELD * PIECE) + s * BLOCK, BLOCK), BLOCK)

    def slot(owner):
        return pl.ds(pl.multiple_of(owner * BLOCK, BLOCK), BLOCK)

    def send_in(to, s):
        pltpu.make_async_remote_copy(
            src_ref=nm_ref.at[block(to, s)],
            dst_ref=taken.at[s, slot(me)],
            send_sem=in_send.at[s],
            recv_sem=in_recv.at[s],
            device_id={"rows": to},
            device_id_type=MESH,
        ).start()

    for dz in range(1, DEPTH // 2 + 1):
        if dz > 1:
            hear()
            if dz < DEPTH // 2:
                tell()

        @pl.loop(0, PLANE)
        def _(j, dz=dz):
            send_in(away(dz, j), 0)
            if dz < DEPTH // 2:
                send_in(away(DEPTH - dz, j), 0)

        if dz == 1:

            @pl.loop(1, PLANE)
            def _(j):
                send_in(away(0, j), 0)

    for s in range(1, STAGES):

        @pl.loop(1, ROWS)
        def _(j, s=s):
            send_in(peer(j, STEPS[s % 2]), s)

    for s in range(STAGES):
        taken[s, slot(me), :] = nm_ref[block(me, s), :]

    def wait_all(ref, rows, sem):
        at = ref.at[pl.ds(0, rows)]
        pltpu.make_async_copy(at, at, sem).wait()

    def grams(s):
        wait_all(taken.at[s], (ROWS - 1) * BLOCK, in_recv.at[s])
        for i in range(PER):
            k = s * PER + i
            for t in range(TILES):
                for r in range(2):
                    whole[k, pl.ds(r * ROWS, ROWS), pl.ds(t * LANES, LANES)] = taken[
                        s, pl.ds(i * PIECE + 2 * t + r, ROWS, stride=BLOCK), :
                    ]
            x = whole[k]
            gram = dot(x, x, (((1,), (1,)), ((), ())))

            @pl.when(col == k)
            def _():
                parts[k] = gram

            @pl.when(col != k)
            def _():
                part[k] = gram
                pltpu.make_async_remote_copy(
                    src_ref=part.at[k],
                    dst_ref=parts.at[col],
                    send_sem=part_send,
                    recv_sem=part_recv,
                    device_id={"cols": k},
                    device_id_type=MESH,
                ).start()

    def mix(s):
        @pl.when(col // PER == s)
        def _():
            wait_all(part, COLS - 1, part_recv)
            mixer[col] = mixing((parts[0] + parts[1]) + (parts[2] + parts[3]))
            for d in range(1, COLS):
                pltpu.make_async_remote_copy(
                    src_ref=mixer.at[col],
                    dst_ref=mixer.at[col],
                    send_sem=mix_send,
                    recv_sem=mix_recv.at[col],
                    device_id={"cols": (col + d) % COLS},
                    device_id_type=MESH,
                ).start()

    def give(s):
        for i in range(PER):
            k = s * PER + i

            @pl.when(col != k)
            def _():
                pltpu.make_async_copy(mixer.at[k], mixer.at[k], mix_recv.at[k]).wait()

            out = dot(mixer[k], whole[k])
            for t in range(TILES):
                for r in range(2):
                    spread[s, pl.ds(i * PIECE + 2 * t + r, ROWS, stride=BLOCK), :] = out[
                        r * ROWS : (r + 1) * ROWS, t * LANES : (t + 1) * LANES
                    ]

        def send_out(to):
            pltpu.make_async_remote_copy(
                src_ref=spread.at[s, slot(to)],
                dst_ref=back.at[block(me, s)],
                send_sem=out_send.at[s],
                recv_sem=out_recv.at[s],
                device_id={"rows": to},
                device_id_type=MESH,
            ).start()

        if s < STAGES - 1:

            @pl.loop(1, ROWS)
            def _(j):
                send_out(peer(j, STEPS[s % 2]))
        else:
            for planes in ((0, 1), (2, 3, 4, 5, 6, 7)):

                @pl.loop(0, PLANE)
                def _(j, planes=planes):
                    for plane in planes:
                        to = plane * PLANE + (me + j) % PLANE

                        @pl.when(to != me)
                        def _(to=to):
                            send_out(to)

        back[block(me, s), :] = spread[s, slot(me), :]

    for s in range(STAGES):
        grams(s)
        mix(s)
        give(s)

    loads[2].wait()
    for s in range(STAGES):
        wait_all(back, (ROWS - 1) * BLOCK, out_recv.at[s])

        def decay(r, carry, s=s):
            at = block(r, s)
            nw_ref[at, :] = (1.0 - learn_rate * decay_rate) * w_buf[at, :] - learn_rate * back[at, :]
            return carry

        lax.fori_loop(0, ROWS, decay, 0, unroll=4)

    for s in range(STAGES):
        wait_all(back, (ROWS - 1) * BLOCK, in_send.at[s])
        wait_all(back, (ROWS - 1) * BLOCK, out_send.at[s])
    wait_all(part, COLS - 1, part_send)
    wait_all(part, COLS - 1, mix_send)


def store(nw_ref, nm_ref, nw_hbm, nm_hbm, sem):
    copies = [
        pltpu.make_async_copy(nw_ref, nw_hbm, sem.at[0]),
        pltpu.make_async_copy(nm_ref, nm_hbm, sem.at[1]),
    ]
    for copy in copies:
        copy.start()
    for copy in copies:
        copy.wait()


def flat(a):
    return a.reshape(ROWS * HELD, 2, TILES, LANES).transpose(0, 2, 1, 3).reshape(FLAT, LANES)


def square(a):
    return a.reshape(ROWS * HELD, TILES, 2, LANES).transpose(0, 2, 1, 3).reshape(ROWS * HELD, 2, TILES * LANES)


def local(gradients, momentum, weights):
    f32 = jnp.float32
    in_hbm = [pltpu.with_memory_space_constraint(flat(a), pltpu.HBM) for a in (gradients, momentum, weights)]
    vmem = pltpu.VMEM
    dma = pltpu.SemaphoreType.DMA
    new_weights, new_momentum = pl.pallas_call(
        kernel,
        out_shape=[pltpu.VMEM((FLAT, LANES), f32)] * 2,
        in_specs=[pl.BlockSpec(memory_space=pltpu.HBM)] * 3,
        scratch_shapes=[
            vmem((FLAT, LANES), f32),
            vmem((FLAT, LANES), f32),
            vmem((FLAT, LANES), f32),
            vmem((STAGES, ROWS * BLOCK, LANES), f32),
            vmem((STAGES, ROWS * BLOCK, LANES), f32),
            vmem((FLAT, LANES), f32),
            vmem((HELD, SIDE, TILES * LANES), f32),
            vmem((HELD, SIDE, SIDE), f32),
            vmem((COLS, SIDE, SIDE), f32),
            vmem((HELD, SIDE, SIDE), f32),
            dma((3,)),
            dma((STAGES,)),
            dma((STAGES,)),
            dma((STAGES,)),
            dma((STAGES,)),
            dma(()),
            dma(()),
            dma(()),
            dma((HELD,)),
            pltpu.SemaphoreType.REGULAR,
            pltpu.SemaphoreType.REGULAR,
        ],
        compiler_params=pltpu.CompilerParams(
            collective_id=0, has_side_effects=True, vmem_limit_bytes=40 * 2**20
        ),
        name="step",
    )(*in_hbm)
    new_weights, new_momentum = pl.pallas_call(
        store,
        out_shape=[jax.ShapeDtypeStruct((FLAT, LANES), f32)] * 2,
        in_specs=[pl.BlockSpec(memory_space=pltpu.VMEM)] * 2,
        out_specs=[pl.BlockSpec(memory_space=pl.ANY)] * 2,
        scratch_shapes=[dma((2,))],
        compiler_params=pltpu.CompilerParams(vmem_limit_bytes=2**20),
        name="store",
    )(new_weights, new_momentum)
    return square(new_weights), square(new_momentum)


def solution(mesh):
    placed = P(None, "rows", "cols")
    return jax.shard_map(
        local, mesh=mesh, in_specs=(placed, placed, placed), out_specs=(placed, placed), check_vma=False
    )
```

```python
import functools

import jax
import jax.numpy as jnp
from jax import lax
from jax.experimental import pallas as pl
from jax.experimental.pallas import tpu as pltpu
from jax.sharding import PartitionSpec as P

ITERS = 4
hold_rate = 0.8
learn_rate = 0.8
decay_rate = 0.1

MESH = pl.DeviceIdType.MESH
HIGHEST = lax.Precision.HIGHEST

DEPTH = 8
PLANE = 8
ROWS = DEPTH * PLANE
COLS = 4
SIDE = 128
LANES = 128
TILES = 8
PIECE = 2 * TILES
HELD = 4
STAGES = 4
PER = HELD // STAGES
BLOCK = PER * PIECE
FLAT = ROWS * HELD * PIECE
STEPS = (13, 37)


def dot(a, b, dims=(((1,), (0,)), ((), ()))):
    return lax.dot_general(a, b, dims, precision=HIGHEST, preferred_element_type=jnp.float32)


def mixing(gram):
    row = lax.broadcasted_iota(jnp.int32, (SIDE, SIDE), 0)
    col = lax.broadcasted_iota(jnp.int32, (SIDE, SIDE), 1)
    eye = row == col
    total = jnp.sum(jnp.sum(jnp.where(eye, gram, 0.0), axis=1, keepdims=True), axis=0, keepdims=True)
    scale = lax.rsqrt(total + 1e-06)
    a = gram * scale * scale
    q = None
    for step in range(ITERS):
        b = -4.775 * a + 2.0315 * dot(a, a)
        if q is None:
            q = (jnp.where(eye, 3.4445, 0.0) + b) * scale
        else:
            q = 3.4445 * q + dot(b, q)
        if step < ITERS - 1:
            half = 3.4445 * a + dot(a, b)
            a = 3.4445 * half + dot(b, half)
    return q


def kernel(
    g_hbm, m_hbm, w_hbm, nw_ref, nm_ref,
    g_buf, m_buf, w_buf, taken, spread, back, whole, part, parts, mixer,
    load_sem, in_send, in_recv, out_send, out_recv, part_send, part_recv, mix_send, mix_recv, below, above,
):
    me = lax.axis_index("rows")
    col = lax.axis_index("cols")
    z, y, core = me // 8, (me // 2) % 4, me % 2

    def peer(j, step):
        off = (j * step) % ROWS
        dz, dy, dc = off // 8, (off // 2) % 4, off % 2
        return ((z + dz) % 8) * 8 + ((y + dy) % 4) * 2 + (core + dc) % 2

    half = FLAT // 2
    loads = []
    for i, (src, dst) in enumerate(((g_hbm, g_buf), (m_hbm, m_buf), (w_hbm, w_buf))):
        load = pltpu.make_async_copy(src, dst, load_sem.at[i])
        load.start()
        loads.append(load)

    barrier = pltpu.get_barrier_semaphore()

    def away(dz, j):
        return ((z + dz) % DEPTH) * PLANE + (me + j) % PLANE

    def greet(dz, j):
        pl.semaphore_signal(barrier, inc=1, device_id={"rows": away(dz, j)}, device_id_type=MESH)

    @pl.loop(0, PLANE)
    def _(j):
        greet(DEPTH - 1, j)
        greet(1, j)

    @pl.loop(1, PLANE)
    def _(j):
        greet(0, j)

    for d in range(1, COLS):
        pl.semaphore_signal(barrier, inc=1, device_id={"cols": (col + d) % COLS}, device_id_type=MESH)

    loads[0].wait()
    loads[1].wait()

    def hold(i, carry):
        at = pl.ds(pl.multiple_of(i * 64, 64), 64)
        nm_ref[at, :] = hold_rate * m_buf[at, :] + g_buf[at, :]
        return carry

    lax.fori_loop(0, FLAT // 64, hold, 0, unroll=4)

    pl.semaphore_wait(barrier, 3 * PLANE - 1 + COLS - 1)

    def tell():
        pl.semaphore_signal(below, inc=1, device_id={"rows": away(1, 0)}, device_id_type=MESH)
        pl.semaphore_signal(above, inc=1, device_id={"rows": away(DEPTH - 1, 0)}, device_id_type=MESH)

    def hear():
        pl.semaphore_wait(below, 1)
        pl.semaphore_wait(above, 1)

    tell()

    def block(owner, s):
        return pl.ds(pl.multiple_of(owner * (HELD * PIECE) + s * BLOCK, BLOCK), BLOCK)

    def slot(owner):
        return pl.ds(pl.multiple_of(owner * BLOCK, BLOCK), BLOCK)

    def send_in(to, s):
        pltpu.make_async_remote_copy(
            src_ref=nm_ref.at[block(to, s)],
            dst_ref=taken.at[s, slot(me)],
            send_sem=in_send.at[s],
            recv_sem=in_recv.at[s],
            device_id={"rows": to},
            device_id_type=MESH,
        ).start()

    for dz in range(1, DEPTH // 2 + 1):
        if dz > 1:
            hear()
            if dz < DEPTH // 2:
                tell()

        @pl.loop(0, PLANE)
        def _(j, dz=dz):
            send_in(away(dz, j), 0)
            if dz < DEPTH // 2:
                send_in(away(DEPTH - dz, j), 0)

        if dz == 1:

            @pl.loop(1, PLANE)
            def _(j):
                send_in(away(0, j), 0)

    for s in range(1, STAGES):

        @pl.loop(1, ROWS)
        def _(j, s=s):
            send_in(peer(j, STEPS[s % 2]), s)

    for s in range(STAGES):
        taken[s, slot(me), :] = nm_ref[block(me, s), :]

    def wait_all(ref, rows, sem):
        at = ref.at[pl.ds(0, rows)]
        pltpu.make_async_copy(at, at, sem).wait()

    def grams(s):
        wait_all(taken.at[s], (ROWS - 1) * BLOCK, in_recv.at[s])
        for i in range(PER):
            k = s * PER + i
            for t in range(TILES):
                for r in range(2):
                    whole[k, pl.ds(r * ROWS, ROWS), pl.ds(t * LANES, LANES)] = taken[
                        s, pl.ds(i * PIECE + 2 * t + r, ROWS, stride=BLOCK), :
                    ]
            x = whole[k]
            gram = dot(x, x, (((1,), (1,)), ((), ())))

            @pl.when(col == k)
            def _():
                parts[k] = gram

            @pl.when(col != k)
            def _():
                part[k] = gram
                pltpu.make_async_remote_copy(
                    src_ref=part.at[k],
                    dst_ref=parts.at[col],
                    send_sem=part_send,
                    recv_sem=part_recv,
                    device_id={"cols": k},
                    device_id_type=MESH,
                ).start()

    def mix(s):
        @pl.when(col // PER == s)
        def _():
            wait_all(part, COLS - 1, part_recv)
            mixer[col] = mixing((parts[0] + parts[1]) + (parts[2] + parts[3]))
            for d in range(1, COLS):
                pltpu.make_async_remote_copy(
                    src_ref=mixer.at[col],
                    dst_ref=mixer.at[col],
                    send_sem=mix_send,
                    recv_sem=mix_recv.at[col],
                    device_id={"cols": (col + d) % COLS},
                    device_id_type=MESH,
                ).start()

    def give(s):
        for i in range(PER):
            k = s * PER + i

            @pl.when(col != k)
            def _():
                pltpu.make_async_copy(mixer.at[k], mixer.at[k], mix_recv.at[k]).wait()

            out = dot(mixer[k], whole[k])
            for t in range(TILES):
                for r in range(2):
                    spread[s, pl.ds(i * PIECE + 2 * t + r, ROWS, stride=BLOCK), :] = out[
                        r * ROWS : (r + 1) * ROWS, t * LANES : (t + 1) * LANES
                    ]

        def send_out(to):
            pltpu.make_async_remote_copy(
                src_ref=spread.at[s, slot(to)],
                dst_ref=back.at[block(me, s)],
                send_sem=out_send.at[s],
                recv_sem=out_recv.at[s],
                device_id={"rows": to},
                device_id_type=MESH,
            ).start()

        if s < STAGES - 1:

            @pl.loop(1, ROWS)
            def _(j):
                send_out(peer(j, STEPS[s % 2]))
        else:
            for planes in ((0, 1), (2, 3, 7), (4, 5, 6)):

                @pl.loop(0, PLANE)
                def _(j, planes=planes):
                    for plane in planes:
                        to = plane * PLANE + (me + j) % PLANE

                        @pl.when(to != me)
                        def _(to=to):
                            send_out(to)

        back[block(me, s), :] = spread[s, slot(me), :]

    for s in range(STAGES):
        grams(s)
        mix(s)
        give(s)

    loads[2].wait()
    for s in range(STAGES):
        wait_all(back, (ROWS - 1) * BLOCK, out_recv.at[s])

        def decay(r, carry, s=s):
            at = block(r, s)
            nw_ref[at, :] = (1.0 - learn_rate * decay_rate) * w_buf[at, :] - learn_rate * back[at, :]
            return carry

        lax.fori_loop(0, ROWS, decay, 0, unroll=4)

    for s in range(STAGES):
        wait_all(back, (ROWS - 1) * BLOCK, in_send.at[s])
        wait_all(back, (ROWS - 1) * BLOCK, out_send.at[s])
    wait_all(part, COLS - 1, part_send)
    wait_all(part, COLS - 1, mix_send)


def store(nw_ref, nm_ref, nw_hbm, nm_hbm, sem):
    copies = [
        pltpu.make_async_copy(nw_ref, nw_hbm, sem.at[0]),
        pltpu.make_async_copy(nm_ref, nm_hbm, sem.at[1]),
    ]
    for copy in copies:
        copy.start()
    for copy in copies:
        copy.wait()


def flat(a):
    return a.reshape(ROWS * HELD, 2, TILES, LANES).transpose(0, 2, 1, 3).reshape(FLAT, LANES)


def square(a):
    return a.reshape(ROWS * HELD, TILES, 2, LANES).transpose(0, 2, 1, 3).reshape(ROWS * HELD, 2, TILES * LANES)


def local(gradients, momentum, weights):
    f32 = jnp.float32
    in_hbm = [pltpu.with_memory_space_constraint(flat(a), pltpu.HBM) for a in (gradients, momentum, weights)]
    vmem = pltpu.VMEM
    dma = pltpu.SemaphoreType.DMA
    new_weights, new_momentum = pl.pallas_call(
        kernel,
        out_shape=[pltpu.VMEM((FLAT, LANES), f32)] * 2,
        in_specs=[pl.BlockSpec(memory_space=pltpu.HBM)] * 3,
        scratch_shapes=[
            vmem((FLAT, LANES), f32),
            vmem((FLAT, LANES), f32),
            vmem((FLAT, LANES), f32),
            vmem((STAGES, ROWS * BLOCK, LANES), f32),
            vmem((STAGES, ROWS * BLOCK, LANES), f32),
            vmem((FLAT, LANES), f32),
            vmem((HELD, SIDE, TILES * LANES), f32),
            vmem((HELD, SIDE, SIDE), f32),
            vmem((COLS, SIDE, SIDE), f32),
            vmem((HELD, SIDE, SIDE), f32),
            dma((3,)),
            dma((STAGES,)),
            dma((STAGES,)),
            dma((STAGES,)),
            dma((STAGES,)),
            dma(()),
            dma(()),
            dma(()),
            dma((HELD,)),
            pltpu.SemaphoreType.REGULAR,
            pltpu.SemaphoreType.REGULAR,
        ],
        compiler_params=pltpu.CompilerParams(
            collective_id=0, has_side_effects=True, vmem_limit_bytes=40 * 2**20
        ),
        name="step",
    )(*in_hbm)
    new_weights, new_momentum = pl.pallas_call(
        store,
        out_shape=[jax.ShapeDtypeStruct((FLAT, LANES), f32)] * 2,
        in_specs=[pl.BlockSpec(memory_space=pltpu.VMEM)] * 2,
        out_specs=[pl.BlockSpec(memory_space=pl.ANY)] * 2,
        scratch_shapes=[dma((2,))],
        compiler_params=pltpu.CompilerParams(vmem_limit_bytes=2**20),
        name="store",
    )(new_weights, new_momentum)
    return square(new_weights), square(new_momentum)


def solution(mesh):
    placed = P(None, "rows", "cols")
    return jax.shard_map(
        local, mesh=mesh, in_specs=(placed, placed, placed), out_specs=(placed, placed), check_vma=False
    )
```
